32 devices in a mesh: seq: 8 (over y, x, core), head: 4 (over z).
Axes of the slice: x: 2, y: 2, z: 4, core: 2. Of those that a mesh axis runs over, the one named last changes fastest.
Arguments:
- queries: bfloat16 [1536, 2048], P('seq', 'head'), may hold values from -6 to 6, as said below
- keys: bfloat16 [1536, 256], P('seq'), may hold values from -6 to 6, as said below
- values: bfloat16 [1536, 256], P('seq'), may hold values from -6 to 6
- out_weight: bfloat16 [2048, 8192], P('head'), may hold values from -0.25 to 0.25
- doc_lengths: int32 [48], replicated, may hold values from 1 to 384, 1536 in all
- pair_ids: int32 [48], replicated, may hold values from 0 to 23, never falling along the last dimension, each value on 1 to 3 neighbouring positions
- block_plan: int32 [32], replicated, may hold values from 0 to 31, as said below
Outputs:
- projected: bfloat16 [1536, 8192], P(('seq', 'head'))
The draws below stay inside these ranges and needn't reach their ends.
Inputs may be any that keep to these rules, and one draw needn't show every extreme that they name: Entries of queries lie in the range given. Entries of keys lie in the range given. `doc_lengths`: the lengths sum to 1536. `pair_ids`: never falling; every pair 0 to 23 holds one to three consecutive documents. `block_plan`: A permutation of the 32 blocks of 48 tokens, numbered along the row. The 4 consecutive slots of one seq index hold blocks from 4 different seq indices, and the 4 blocks of one seq index go to 4 different seq indices.
All inputs are finite; a program needn't handle non-finite values.
Results may differ from the reference program's by a relative error of at most 0.015.
Values may be sent and summed in bfloat16 or wider, within the bound.
A program may use at most 64 MiB of HBM per device.

```python
import math
import jax
import jax.numpy as jnp
import numpy as np
from jax import lax

D = 8192
D_HEAD = 128
QH_DEV = 4
TOK_DEV = 192
NDOC = 48
NPAIR = 24
KV_HEADS = 2
Q_HEADS = 16
NB = 4
BLK = 48
NBLK = 32
SEQ_LEN = 1536
MAXDOC = 384


def paired_rows(key):
    query_key, keys_key = jax.random.split(jax.random.fold_in(key, 31), 2)
    query_width = Q_HEADS * D_HEAD
    key_width = KV_HEADS * D_HEAD
    query_vals = jnp.clip(jax.random.normal(query_key, (SEQ_LEN, query_width), jnp.float32), -6.0, 6.0)
    key_vals = jnp.clip(jax.random.normal(keys_key, (SEQ_LEN, key_width), jnp.float32), -6.0, 6.0)
    return (query_vals, key_vals)


def draw_queries(key, part):
    return paired_rows(key)[0].astype(jnp.bfloat16)


def draw_keys(key, part):
    return paired_rows(key)[1].astype(jnp.bfloat16)


def draw_block_plan(key, part):
    device_count = SEQ_LEN // TOK_DEV
    first_key, second_key, third_key, fourth_key = jax.random.split(jax.random.fold_in(key, 53), 4)
    offsets = jax.random.permutation(first_key, device_count)[:NB].astype(jnp.int32)
    outer = jax.random.permutation(second_key, device_count).astype(jnp.int32)
    inner = jax.random.permutation(third_key, device_count).astype(jnp.int32)
    local_order = jax.random.permutation(fourth_key, NB).astype(jnp.int32)
    outer_inverse = jnp.argsort(outer).astype(jnp.int32)
    inner_inverse = jnp.argsort(inner).astype(jnp.int32)
    shifted = (outer_inverse[:, None] - offsets[None, :]) % device_count
    source = inner_inverse[shifted]
    plan = source * NB + local_order[None, :]
    return plan.reshape(-1).astype(jnp.int32)


def block_levels(stream_key, shape, cuts, low, high):
    def one(axis_at, shards_of):
        draws = jax.random.uniform(jax.random.fold_in(jax.random.fold_in(stream_key, 6), axis_at), (shards_of,), jnp.float32, low / len(cuts), high / len(cuts))
        return jnp.repeat(jnp.exp(draws), shape[axis_at] // shards_of).reshape((-1,) + (1,) * (len(shape) - axis_at - 1))

    level = one(*cuts[0])
    for cut in cuts[1:]:
        level = level * one(*cut)
    return level


def profile(amount, total, most, lean):
    weights = [(1 << 20) // math.isqrt(rank ** lean) + 1 for rank in range(2, amount + 1)]
    surplus, holding = total - most - (amount - 1), [1] * (amount - 1)
    while surplus > 0:
        movable = [i for i in range(amount - 1) if holding[i] < most]
        mass, budget = sum([weights[i] for i in movable]), surplus
        for i in movable:
            more = min(most - holding[i], max(1, budget * weights[i] // mass), surplus)
            holding[i] = holding[i] + more
            surplus = surplus - more
    return np.array([most] + holding)


def ragged(stream_key, count, total, bound, slope):
    if count == 2:
        one = jax.random.randint(stream_key, (), max(1, total - bound), min(bound, total - 1) + 1)
        return jnp.stack([one, total - one])
    lengths = jnp.asarray(profile(count, total, bound, slope), jnp.int32)
    pairs = (count - 1) // 2
    donor, receiver = lengths[1:1 + 2 * pairs:2], lengths[2:2 + 2 * pairs:2]
    room = jnp.minimum(donor - 1, bound - receiver)
    passed = jax.random.randint(jax.random.fold_in(stream_key, 1), (pairs,), 0, 1 << 20) % (room + 1)
    lengths = lengths.at[1:1 + 2 * pairs:2].set(donor - passed).at[2:2 + 2 * pairs:2].set(receiver + passed)
    return lengths[jax.random.permutation(jax.random.fold_in(stream_key, 2), count)]


def normal_values(own_key, extent, deviation, reach, cuts=(), kind=jnp.bfloat16):
    array = deviation * jax.random.normal(own_key, extent, jnp.float32)
    if cuts:
        array = array * block_levels(own_key, extent, cuts, -0.22, 0.18)
    return jnp.clip(array, -reach, reach).astype(kind)


def setup_inputs(seed: int = 0) -> dict:
    seeds = jax.random.split(jax.random.key(seed), 8)
    queries = draw_queries(jax.random.fold_in(seeds[7], 71), 0)
    keys = draw_keys(jax.random.fold_in(seeds[7], 71), 0)
    values = normal_values(seeds[2], (SEQ_LEN, KV_HEADS * D_HEAD), 1.0, 6.0, ((0, 8),))
    out_weight = normal_values(seeds[3], (Q_HEADS * D_HEAD, D), (QH_DEV * D_HEAD) ** -0.5, 0.25, ((0, 4),))
    doc_lengths = ragged(seeds[4], NDOC, SEQ_LEN, MAXDOC, 2).astype(jnp.int32)
    pair_ids = jnp.searchsorted(jnp.cumsum(ragged(seeds[5], NPAIR, NDOC, 3, 0)), jnp.arange(NDOC), side="right").astype(jnp.int32)
    block_plan = draw_block_plan(jax.random.fold_in(seeds[7], 71), 0)
    return {"queries": queries, "keys": keys, "values": values, "out_weight": out_weight, "doc_lengths": doc_lengths, "pair_ids": pair_ids, "block_plan": block_plan}


NEGATIVE = -1e+30

def token_docs(positions, doc_lengths):
    doc_ends = jnp.cumsum(doc_lengths)
    return lax.optimization_barrier(jnp.sum((doc_ends[None, :] <= positions[:, None]).astype(jnp.int32), axis=1))

def pair_firsts(docs, pair_ids):
    doc_range = jnp.arange(pair_ids.shape[0], dtype=jnp.int32)
    own_pair = lax.optimization_barrier(jnp.sum(jnp.where(docs[:, None] == doc_range[None, :], pair_ids[None, :], 0), axis=1))
    return lax.optimization_barrier(jnp.sum((pair_ids[None, :] < own_pair[:, None]).astype(jnp.int32), axis=1))

def reference(queries, keys, values, out_weight, doc_lengths, pair_ids, block_plan):
    positions = jnp.arange(SEQ_LEN, dtype=jnp.int32)
    docs_all = token_docs(positions, doc_lengths)
    firsts_all = pair_firsts(docs_all, pair_ids)
    scale = 1.0 / math.sqrt(D_HEAD)
    query_block = 4 * TOK_DEV
    block_total = SEQ_LEN // query_block
    group_total = Q_HEADS // QH_DEV

    def one_group(group_index):
        kv_index = group_index // 2
        key_rows = lax.dynamic_slice_in_dim(keys, (kv_index * D_HEAD).astype(jnp.int32), D_HEAD, 1).astype(jnp.float32)
        value_rows = lax.dynamic_slice_in_dim(values, (kv_index * D_HEAD).astype(jnp.int32), D_HEAD, 1).astype(jnp.float32)
        group_queries = lax.dynamic_slice_in_dim(queries, (group_index * QH_DEV * D_HEAD).astype(jnp.int32), QH_DEV * D_HEAD, 1)

        def one_block(block_index):
            start_row = (block_index * query_block).astype(jnp.int32)
            query_rows = lax.dynamic_slice_in_dim(group_queries, start_row, query_block, 0)
            query_rows = query_rows.astype(jnp.float32).reshape(query_block, QH_DEV, D_HEAD)
            row_pos = lax.dynamic_slice_in_dim(positions, start_row, query_block, 0)
            row_docs = lax.dynamic_slice_in_dim(docs_all, start_row, query_block, 0)
            row_firsts = lax.dynamic_slice_in_dim(firsts_all, start_row, query_block, 0)
            allowed = (positions[None, :] <= row_pos[:, None]) & ((docs_all[None, :] == row_docs[:, None]) | (docs_all[None, :] == row_firsts[:, None]))
            scores = jnp.einsum('qhd,kd->hqk', query_rows, key_rows) * scale
            row_max = lax.optimization_barrier(jnp.max(jnp.where(allowed[None], scores, NEGATIVE), axis=2))
            weights = jnp.where(allowed[None], jnp.exp(scores - row_max[:, :, None]), 0.0)
            denominator = lax.optimization_barrier(jnp.sum(weights, axis=2))
            rounded = lax.optimization_barrier(weights.astype(jnp.bfloat16)).astype(jnp.float32)
            combined = jnp.einsum('hqk,kd->hqd', rounded, value_rows) / denominator[:, :, None]
            return combined.transpose(1, 0, 2).reshape(query_block, QH_DEV * D_HEAD).astype(jnp.bfloat16)
        outputs = lax.map(one_block, jnp.arange(block_total, dtype=jnp.int32))
        return outputs.reshape(SEQ_LEN, QH_DEV * D_HEAD)
    grouped = lax.map(one_group, jnp.arange(group_total, dtype=jnp.int32))
    attended = grouped.transpose(1, 0, 2).reshape(SEQ_LEN, group_total * QH_DEV * D_HEAD)
    planned = attended.reshape(NBLK, BLK, group_total * QH_DEV * D_HEAD)[block_plan]
    planned = planned.reshape(SEQ_LEN, group_total, QH_DEV * D_HEAD)
    weight_groups = out_weight.reshape(group_total, QH_DEV * D_HEAD, D)

    def add_group(running_total, group_index):
        group_rows = lax.dynamic_index_in_dim(planned, group_index, 1, False)
        group_weight = lax.dynamic_index_in_dim(weight_groups, group_index, 0, False)
        partial_term = jnp.dot(group_rows, group_weight, preferred_element_type=jnp.float32).astype(jnp.bfloat16)
        return (running_total + lax.optimization_barrier(partial_term).astype(jnp.float32), None)
    summed, unused_out = lax.scan(add_group, jnp.zeros((SEQ_LEN, D), jnp.float32), jnp.arange(group_total, dtype=jnp.int32))
    return summed.astype(jnp.bfloat16)
```

```python
import functools
import math

import jax
import jax.numpy as jnp
from jax import lax
from jax.experimental import pallas as pl
from jax.experimental.pallas import tpu as pltpu
from jax.sharding import PartitionSpec as P

D_HEAD = 128


NEGATIVE = -1e30


def token_docs(positions, doc_lengths):
    doc_ends = jnp.cumsum(doc_lengths)
    return jnp.sum((doc_ends[None, :] <= positions[:, None]).astype(jnp.int32), axis=1)


def pair_firsts(docs, pair_ids):
    doc_range = jnp.arange(pair_ids.shape[0], dtype=jnp.int32)
    own_pair = jnp.sum(jnp.where(docs[:, None] == doc_range[None, :], pair_ids[None, :], 0), axis=1)
    return jnp.sum((pair_ids[None, :] < own_pair[:, None]).astype(jnp.int32), axis=1)


def largest_divisor(total_rows, ceiling):
    return max(
        (
            candidate
            for candidate in range(1, min(total_rows, ceiling) + 1)
            if total_rows % candidate == 0
        )
    )


def attend(query_rows, positions, keys, values, doc_lengths, pair_ids):
    head_size = keys.shape[1]
    token_count = query_rows.shape[0]
    query_heads = query_rows.shape[1] // head_size
    shaped_queries = query_rows.reshape(token_count, query_heads, head_size)
    query_docs = token_docs(positions, doc_lengths)
    query_firsts = pair_firsts(query_docs, pair_ids)
    doc_range = jnp.arange(doc_lengths.shape[0], dtype=jnp.int32)
    pair_begin = jnp.sum(
        jnp.where(doc_range[None, :] < query_firsts[:, None], doc_lengths[None, :], 0), axis=1
    )
    lowest = jnp.min(pair_begin)
    highest = jnp.max(positions)
    scale = 1.0 / math.sqrt(head_size)

    def update(softmax_state, key_block, value_block, block_start):
        key_pos = block_start + jnp.arange(key_block.shape[0], dtype=jnp.int32)
        needed = (block_start <= highest) & (block_start + key_block.shape[0] > lowest)

        def compute(current):
            running_max, denominator, weighted = current
            key_docs = token_docs(key_pos, doc_lengths)
            allowed = (key_pos[None, :] <= positions[:, None]) & (
                (key_docs[None, :] == query_docs[:, None])
                | (key_docs[None, :] == query_firsts[:, None])
            )
            scores = (
                jnp.einsum(
                    "qhd,kd->hqk", shaped_queries, key_block, preferred_element_type=jnp.float32
                )
                * scale
            )
            newest = jnp.maximum(
                running_max, jnp.max(jnp.where(allowed[None], scores, NEGATIVE), axis=2)
            )
            weights = jnp.where(allowed[None], jnp.exp(scores - newest[:, :, None]), 0.0)
            factor = jnp.exp(running_max - newest)
            denominator = denominator * factor + jnp.sum(weights, axis=2)
            weighted = weighted * factor[:, :, None] + jnp.einsum(
                "hqk,kd->hqd",
                weights.astype(jnp.bfloat16),
                value_block,
                preferred_element_type=jnp.float32,
            )
            return (newest, denominator, weighted)

        def unchanged(current):
            return current

        return lax.cond(needed, compute, unchanged, softmax_state)

    initial = (
        jnp.full((query_heads, token_count), NEGATIVE, jnp.float32),
        jnp.zeros((query_heads, token_count), jnp.float32),
        jnp.zeros((query_heads, token_count, head_size), jnp.float32),
    )
    key_rows = lax.all_gather(keys, "seq", axis=0, tiled=True)
    value_rows = lax.all_gather(values, "seq", axis=0, tiled=True)
    row_total = key_rows.shape[0]
    block_rows = largest_divisor(row_total, 1024)
    block_count = row_total // block_rows
    stacked = (
        key_rows.reshape(block_count, block_rows, head_size),
        value_rows.reshape(block_count, block_rows, head_size),
        jnp.int32(0) + block_rows * jnp.arange(block_count, dtype=jnp.int32),
    )

    def advance(carried, block_item):
        return (update(carried, block_item[0], block_item[1], block_item[2]), None)

    result_state, unused_out = lax.scan(advance, initial, stacked)
    running_max, denominator, weighted = result_state
    attended = weighted / denominator[:, :, None]
    return (
        attended.transpose(1, 0, 2)
        .reshape(token_count, query_heads * head_size)
        .astype(jnp.bfloat16)
    )


def on_device(queries, keys, values, out_weight, doc_lengths, pair_ids, block_plan):
    seq_count = lax.axis_size("seq")
    my_seq = lax.axis_index("seq")
    shared_head = lax.axis_index("head") // 2
    key_rows = lax.dynamic_slice_in_dim(keys, shared_head * D_HEAD, D_HEAD, 1)
    value_rows = lax.dynamic_slice_in_dim(values, shared_head * D_HEAD, D_HEAD, 1)
    slots_here = seq_count // 2
    tok_rows = queries.shape[0]
    row_width = queries.shape[1]
    block_rows = tok_rows // slots_here
    slot_total = block_plan.shape[0]
    local_ids = my_seq * slots_here + jnp.arange(slots_here, dtype=jnp.int32)
    plan_rows = lax.dynamic_slice_in_dim(block_plan, my_seq * slots_here, slots_here, 0)
    planned_pos = (
        plan_rows[:, None] * block_rows + jnp.arange(block_rows, dtype=jnp.int32)[None, :]
    ).reshape(-1)
    slot_range = jnp.arange(slot_total, dtype=jnp.int32)
    target_slot = jnp.sum(
        jnp.where(block_plan[None, :] == local_ids[:, None], slot_range[None, :], 0), axis=1
    )
    device_range = jnp.arange(seq_count, dtype=jnp.int32)
    send_table = ((target_slot // slots_here)[:, None] == device_range[None, :]).astype(
        jnp.bfloat16
    )
    take_table = ((plan_rows // slots_here)[:, None] == device_range[None, :]).astype(jnp.bfloat16)
    blocked = queries.reshape(slots_here, block_rows, row_width)
    arrived = lax.all_to_all(
        jnp.einsum("bn,bkw->nkw", send_table, blocked, preferred_element_type=jnp.float32).astype(
            jnp.bfloat16
        ),
        "seq",
        split_axis=0,
        concat_axis=0,
        tiled=True,
    )
    chosen = jnp.einsum("bn,nkw->bkw", take_table, arrived, preferred_element_type=jnp.float32)
    attended = attend(
        chosen.astype(jnp.bfloat16).reshape(tok_rows, row_width),
        planned_pos,
        key_rows,
        value_rows,
        doc_lengths,
        pair_ids,
    )
    return lax.psum_scatter(
        jnp.dot(attended, out_weight, preferred_element_type=jnp.float32).astype(jnp.bfloat16),
        "head",
        scatter_dimension=0,
        tiled=True,
    )


FAR = 1e9


def cut_columns(width):
    return max(c for c in (1, 2, 4, 8) if width % (c * 128) == 0)


def fused_kernel(
    seq_count,
    head_count,
    queries_ref,
    keys_ref,
    values_ref,
    weight_hbm,
    ends_ref,
    lens_ref,
    pairs_ref,
    plan_ref,
    out_ref,
    weight,
    kv_all,
    q_send,
    q_recv,
    q_heads,
    bias,
    attended,
    right_in,
    left_in,
    right_out,
    left_out,
    weight_sem,
    kv_sems,
    q_sems,
    right_sems,
    left_sems,
):
    me = lax.axis_index("seq")
    rank = lax.axis_index("head")
    slots, block_rows, width = queries_ref.shape
    tokens = slots * block_rows
    seq_len = seq_count * tokens
    heads = width // D_HEAD
    shared = head_count // (keys_ref.shape[1] // D_HEAD)
    chunk_rows = tokens // head_count
    tiles = right_in.shape[1]
    tile = right_in.shape[3]

    weight_copy = pltpu.make_async_copy(weight_hbm, weight, weight_sem)
    weight_copy.start()

    barrier = pltpu.get_barrier_semaphore()
    for step in range(1, seq_count):
        pl.semaphore_signal(
            barrier, inc=1, device_id={"seq": lax.rem(me + step, seq_count)}
        )

    @pl.when(rank > 0)
    def _():
        pl.semaphore_signal(barrier, inc=1, device_id={"head": rank - 1})

    @pl.when(rank < head_count - 1)
    def _():
        pl.semaphore_signal(barrier, inc=1, device_id={"head": rank + 1})

    kv_col = pl.ds(pl.multiple_of((rank // shared) * D_HEAD, D_HEAD), D_HEAD)
    kv_all[me, 0] = keys_ref[:, kv_col]
    kv_all[me, 1] = values_ref[:, kv_col]
    for other in range(seq_count):
        local = jnp.int32(0)
        for slot in range(slots):
            offset = plan_ref[other * slots + slot] - me * slots
            local = local + jnp.where((offset >= 0) & (offset < slots), offset, 0)
        q_send[other] = queries_ref[local]
    q_recv[me] = q_send[me]

    edge = jnp.where(rank > 0, 1, 0) + jnp.where(rank < head_count - 1, 1, 0)
    pl.semaphore_wait(barrier, seq_count - 1 + edge)

    def kv_copy(peer, slot):
        return pltpu.make_async_remote_copy(
            src_ref=kv_all.at[slot],
            dst_ref=kv_all.at[slot],
            send_sem=kv_sems.at[0, peer],
            recv_sem=kv_sems.at[1, slot],
            device_id={"seq": peer},
        )

    def q_copy(peer, slot):
        return pltpu.make_async_remote_copy(
            src_ref=q_send.at[peer],
            dst_ref=q_recv.at[slot],
            send_sem=q_sems.at[0, peer],
            recv_sem=q_sems.at[1, slot],
            device_id={"seq": peer},
        )

    for step in range(1, seq_count):
        peer = lax.rem(me + step, seq_count)
        q_copy(peer, me).start()
    for step in range(1, seq_count):
        peer = lax.rem(me + step, seq_count)
        kv_copy(peer, me).start()

    row = lax.broadcasted_iota(jnp.int32, (tokens, 1), 0)
    position = row
    for slot in range(slots):
        shift = (plan_ref[me * slots + slot] - slot) * block_rows
        here = (row >= slot * block_rows) & (row < (slot + 1) * block_rows)
        position = position + jnp.where(here, shift, 0)
    position = position.astype(jnp.float32)
    ends = ends_ref[...].astype(jnp.float32)
    starts = ends - lens_ref[...].astype(jnp.float32)
    pairs = pairs_ref[...].astype(jnp.float32)
    begun = starts <= position
    own_start = jnp.max(jnp.where(begun, starts, 0.0), axis=1, keepdims=True)
    own_pair = jnp.max(jnp.where(begun, pairs, 0.0), axis=1, keepdims=True)
    same = pairs == own_pair
    first_start = jnp.min(jnp.where(same, starts, FAR), axis=1, keepdims=True)
    first_end = jnp.min(jnp.where(same, ends, FAR), axis=1, keepdims=True)
    for part in range(seq_count):
        key_pos = (
            lax.broadcasted_iota(jnp.int32, (tokens, tokens), 1) + part * tokens
        ).astype(jnp.float32)
        seen = (key_pos <= position) & (
            (key_pos >= own_start) | ((key_pos >= first_start) & (key_pos < first_end))
        )
        bias[part] = jnp.where(seen, 0.0, NEGATIVE)

    for step in range(1, seq_count):
        source = lax.rem(me + seq_count - step, seq_count)
        q_copy(source, source).wait_recv()
    for slot in range(slots):
        block = q_recv[plan_ref[me * slots + slot] // slots]
        for head in range(heads):
            q_heads[head, slot * block_rows : (slot + 1) * block_rows, :] = block[
                :, head * D_HEAD : (head + 1) * D_HEAD
            ]
    for step in range(1, seq_count):
        source = lax.rem(me + seq_count - step, seq_count)
        kv_copy(source, source).wait_recv()

    scale = 1.0 / math.sqrt(D_HEAD)

    def one_head(head, carry):
        rows_q = q_heads[head]
        scores = []
        for part in range(seq_count):
            scores.append(
                lax.dot_general(
                    rows_q,
                    kv_all[part, 0],
                    (((1,), (1,)), ((), ())),
                    preferred_element_type=jnp.float32,
                )
                * scale
                + bias[part]
            )
        top = functools.reduce(jnp.maximum, scores)
        top = jnp.max(top, axis=1, keepdims=True)
        total = jnp.zeros((tokens, tokens), jnp.float32)
        summed = jnp.zeros((tokens, D_HEAD), jnp.float32)
        for part in range(seq_count):
            weights = jnp.exp(scores[part] - top)
            total = total + weights
            summed = summed + jnp.dot(
                weights.astype(jnp.bfloat16),
                kv_all[part, 1],
                preferred_element_type=jnp.float32,
            )
        total = jnp.sum(total, axis=1, keepdims=True)
        result = (summed / total).astype(jnp.bfloat16)
        for chunk in range(head_count):
            attended[head, chunk] = result[chunk * chunk_rows : (chunk + 1) * chunk_rows]
        return carry

    lax.fori_loop(0, heads, one_head, 0)
    weight_copy.wait()

    def own_term(chunk, at):
        columns = pl.ds(pl.multiple_of(at * tile, tile), tile)
        rows_a = jnp.concatenate([attended[head, chunk] for head in range(heads)], axis=1)
        return jnp.dot(rows_a, weight[:, columns], preferred_element_type=jnp.float32)

    def right_copy(chunk, at):
        return pltpu.make_async_remote_copy(
            src_ref=right_out.at[chunk, at],
            dst_ref=right_in.at[chunk, at],
            send_sem=right_sems.at[0, chunk, at],
            recv_sem=right_sems.at[1, chunk, at],
            device_id={"head": jnp.minimum(rank + 1, head_count - 1)},
        )

    def left_copy(chunk, at):
        return pltpu.make_async_remote_copy(
            src_ref=left_out.at[chunk, at],
            dst_ref=left_in.at[chunk, at],
            send_sem=left_sems.at[0, chunk, at],
            recv_sem=left_sems.at[1, chunk, at],
            device_id={"head": jnp.maximum(rank - 1, 0)},
        )

    def advance(item, carry):
        step = item // tiles
        at = item - step * tiles
        far = head_count - 1 - step

        @pl.when((far > rank) & (rank == 0))
        def _():
            right_out[far, at] = own_term(far, at).astype(jnp.bfloat16)
            right_copy(far, at).start()

        @pl.when((step < rank) & (rank == head_count - 1))
        def _():
            left_out[step, at] = own_term(step, at).astype(jnp.bfloat16)
            left_copy(step, at).start()

        @pl.when((far > rank) & (rank > 0))
        def _():
            term = own_term(far, at)
            right_copy(far, at).wait_recv()
            right_out[far, at] = (term + right_in[far, at].astype(jnp.float32)).astype(
                jnp.bfloat16
            )
            right_copy(far, at).start()

        @pl.when((step < rank) & (rank < head_count - 1))
        def _():
            term = own_term(step, at)
            left_copy(step, at).wait_recv()
            left_out[step, at] = (term + left_in[step, at].astype(jnp.float32)).astype(
                jnp.bfloat16
            )
            left_copy(step, at).start()

        return carry

    lax.fori_loop(0, (head_count - 1) * tiles, advance, 0)

    def finish(at, carry):
        columns = pl.ds(pl.multiple_of(at * tile, tile), tile)
        term = own_term(rank, at)

        @pl.when(rank == 0)
        def _():
            left_copy(rank, at).wait_recv()
            out_ref[:, columns] = (term + left_in[rank, at].astype(jnp.float32)).astype(
                jnp.bfloat16
            )

        @pl.when(rank == head_count - 1)
        def _():
            right_copy(rank, at).wait_recv()
            out_ref[:, columns] = (term + right_in[rank, at].astype(jnp.float32)).astype(
                jnp.bfloat16
            )

        @pl.when((rank > 0) & (rank < head_count - 1))
        def _():
            right_copy(rank, at).wait_recv()
            left_copy(rank, at).wait_recv()
            out_ref[:, columns] = (
                term
                + right_in[rank, at].astype(jnp.float32)
                + left_in[rank, at].astype(jnp.float32)
            ).astype(jnp.bfloat16)

        return carry

    lax.fori_loop(0, tiles, finish, 0)

    def drain(item, carry):
        step = item // tiles
        at = item - step * tiles

        @pl.when(step > rank)
        def _():
            right_copy(step, at).wait_send()

        @pl.when(step < rank)
        def _():
            left_copy(step, at).wait_send()

        return carry

    lax.fori_loop(0, head_count * tiles, drain, 0)
    for step in range(1, seq_count):
        peer = lax.rem(me + step, seq_count)
        q_copy(peer, me).wait_send()
        kv_copy(peer, me).wait_send()


def fused_device(queries, keys, values, out_weight, doc_lengths, pair_ids, block_plan):
    seq_count = lax.axis_size("seq")
    head_count = lax.axis_size("head")
    tokens, width = queries.shape
    slots = block_plan.shape[0] // seq_count
    block_rows = tokens // slots
    out_width = out_weight.shape[1]
    tiles = cut_columns(out_width)
    tile = out_width // tiles
    chunk_rows = tokens // head_count
    half = jnp.bfloat16
    flow = pltpu.VMEM((head_count, tiles, chunk_rows, tile), half)
    in_vmem = pl.BlockSpec(memory_space=pltpu.VMEM)
    return pl.pallas_call(
        functools.partial(fused_kernel, seq_count, head_count),
        out_shape=jax.ShapeDtypeStruct((chunk_rows, out_width), half),
        in_specs=[
            in_vmem,
            in_vmem,
            in_vmem,
            pl.BlockSpec(memory_space=pl.ANY),
            in_vmem,
            in_vmem,
            in_vmem,
            pl.BlockSpec(memory_space=pltpu.SMEM),
        ],
        out_specs=in_vmem,
        scratch_shapes=[
            pltpu.VMEM(out_weight.shape, half),
            pltpu.VMEM((seq_count, 2, tokens, D_HEAD), half),
            pltpu.VMEM((seq_count, block_rows, width), half),
            pltpu.VMEM((seq_count, block_rows, width), half),
            pltpu.VMEM((width // D_HEAD, tokens, D_HEAD), half),
            pltpu.VMEM((seq_count, tokens, tokens), jnp.float32),
            pltpu.VMEM((width // D_HEAD, head_count, chunk_rows, D_HEAD), half),
            flow,
            flow,
            flow,
            flow,
            pltpu.SemaphoreType.DMA,
            pltpu.SemaphoreType.DMA((2, seq_count)),
            pltpu.SemaphoreType.DMA((2, seq_count)),
            pltpu.SemaphoreType.DMA((2, head_count, tiles)),
            pltpu.SemaphoreType.DMA((2, head_count, tiles)),
        ],
        compiler_params=pltpu.CompilerParams(
            collective_id=0, has_side_effects=True, vmem_limit_bytes=60000 * 1024
        ),
    )(
        queries.reshape(slots, block_rows, width),
        keys,
        values,
        out_weight,
        jnp.cumsum(doc_lengths)[None],
        doc_lengths[None],
        pair_ids[None],
        block_plan,
    )


def pick_device(queries, keys, values, out_weight, doc_lengths, pair_ids, block_plan):
    seq_count = lax.axis_size("seq")
    tokens = queries.shape[0]
    block_rows = tokens * seq_count // block_plan.shape[0]
    fits = seq_count * tokens * tokens * 4 <= 4 * 1024 * 1024
    aligned = block_rows % 16 == 0 and (tokens // lax.axis_size("head")) % 16 == 0
    run = fused_device if fits and aligned else on_device
    return run(queries, keys, values, out_weight, doc_lengths, pair_ids, block_plan)


def solution(mesh):
    return jax.shard_map(
        pick_device,
        mesh=mesh,
        in_specs=(P("seq", "head"), P("seq", None), P("seq", None), P("head", None), P(), P(), P()),
        out_specs=P(("seq", "head"), None),
        check_vma=False,
    )
```

```python
import functools
import math

import jax
import jax.numpy as jnp
from jax import lax
from jax.experimental import pallas as pl
from jax.experimental.pallas import tpu as pltpu
from jax.sharding import PartitionSpec as P

D_HEAD = 128


NEGATIVE = -1e30


def token_docs(positions, doc_lengths):
    doc_ends = jnp.cumsum(doc_lengths)
    return jnp.sum((doc_ends[None, :] <= positions[:, None]).astype(jnp.int32), axis=1)


def pair_firsts(docs, pair_ids):
    doc_range = jnp.arange(pair_ids.shape[0], dtype=jnp.int32)
    own_pair = jnp.sum(jnp.where(docs[:, None] == doc_range[None, :], pair_ids[None, :], 0), axis=1)
    return jnp.sum((pair_ids[None, :] < own_pair[:, None]).astype(jnp.int32), axis=1)


def largest_divisor(total_rows, ceiling):
    return max(
        (
            candidate
            for candidate in range(1, min(total_rows, ceiling) + 1)
            if total_rows % candidate == 0
        )
    )


def attend(query_rows, positions, keys, values, doc_lengths, pair_ids):
    head_size = keys.shape[1]
    token_count = query_rows.shape[0]
    query_heads = query_rows.shape[1] // head_size
    shaped_queries = query_rows.reshape(token_count, query_heads, head_size)
    query_docs = token_docs(positions, doc_lengths)
    query_firsts = pair_firsts(query_docs, pair_ids)
    doc_range = jnp.arange(doc_lengths.shape[0], dtype=jnp.int32)
    pair_begin = jnp.sum(
        jnp.where(doc_range[None, :] < query_firsts[:, None], doc_lengths[None, :], 0), axis=1
    )
    lowest = jnp.min(pair_begin)
    highest = jnp.max(positions)
    scale = 1.0 / math.sqrt(head_size)

    def update(softmax_state, key_block, value_block, block_start):
        key_pos = block_start + jnp.arange(key_block.shape[0], dtype=jnp.int32)
        needed = (block_start <= highest) & (block_start + key_block.shape[0] > lowest)

        def compute(current):
            running_max, denominator, weighted = current
            key_docs = token_docs(key_pos, doc_lengths)
            allowed = (key_pos[None, :] <= positions[:, None]) & (
                (key_docs[None, :] == query_docs[:, None])
                | (key_docs[None, :] == query_firsts[:, None])
            )
            scores = (
                jnp.einsum(
                    "qhd,kd->hqk", shaped_queries, key_block, preferred_element_type=jnp.float32
                )
                * scale
            )
            newest = jnp.maximum(
                running_max, jnp.max(jnp.where(allowed[None], scores, NEGATIVE), axis=2)
            )
            weights = jnp.where(allowed[None], jnp.exp(scores - newest[:, :, None]), 0.0)
            factor = jnp.exp(running_max - newest)
            denominator = denominator * factor + jnp.sum(weights, axis=2)
            weighted = weighted * factor[:, :, None] + jnp.einsum(
                "hqk,kd->hqd",
                weights.astype(jnp.bfloat16),
                value_block,
                preferred_element_type=jnp.float32,
            )
            return (newest, denominator, weighted)

        def unchanged(current):
            return current

        return lax.cond(needed, compute, unchanged, softmax_state)

    initial = (
        jnp.full((query_heads, token_count), NEGATIVE, jnp.float32),
        jnp.zeros((query_heads, token_count), jnp.float32),
        jnp.zeros((query_heads, token_count, head_size), jnp.float32),
    )
    key_rows = lax.all_gather(keys, "seq", axis=0, tiled=True)
    value_rows = lax.all_gather(values, "seq", axis=0, tiled=True)
    row_total = key_rows.shape[0]
    block_rows = largest_divisor(row_total, 1024)
    block_count = row_total // block_rows
    stacked = (
        key_rows.reshape(block_count, block_rows, head_size),
        value_rows.reshape(block_count, block_rows, head_size),
        jnp.int32(0) + block_rows * jnp.arange(block_count, dtype=jnp.int32),
    )

    def advance(carried, block_item):
        return (update(carried, block_item[0], block_item[1], block_item[2]), None)

    result_state, unused_out = lax.scan(advance, initial, stacked)
    running_max, denominator, weighted = result_state
    attended = weighted / denominator[:, :, None]
    return (
        attended.transpose(1, 0, 2)
        .reshape(token_count, query_heads * head_size)
        .astype(jnp.bfloat16)
    )


def on_device(queries, keys, values, out_weight, doc_lengths, pair_ids, block_plan):
    seq_count = lax.axis_size("seq")
    my_seq = lax.axis_index("seq")
    shared_head = lax.axis_index("head") // 2
    key_rows = lax.dynamic_slice_in_dim(keys, shared_head * D_HEAD, D_HEAD, 1)
    value_rows = lax.dynamic_slice_in_dim(values, shared_head * D_HEAD, D_HEAD, 1)
    slots_here = seq_count // 2
    tok_rows = queries.shape[0]
    row_width = queries.shape[1]
    block_rows = tok_rows // slots_here
    slot_total = block_plan.shape[0]
    local_ids = my_seq * slots_here + jnp.arange(slots_here, dtype=jnp.int32)
    plan_rows = lax.dynamic_slice_in_dim(block_plan, my_seq * slots_here, slots_here, 0)
    planned_pos = (
        plan_rows[:, None] * block_rows + jnp.arange(block_rows, dtype=jnp.int32)[None, :]
    ).reshape(-1)
    slot_range = jnp.arange(slot_total, dtype=jnp.int32)
    target_slot = jnp.sum(
        jnp.where(block_plan[None, :] == local_ids[:, None], slot_range[None, :], 0), axis=1
    )
    device_range = jnp.arange(seq_count, dtype=jnp.int32)
    send_table = ((target_slot // slots_here)[:, None] == device_range[None, :]).astype(
        jnp.bfloat16
    )
    take_table = ((plan_rows // slots_here)[:, None] == device_range[None, :]).astype(jnp.bfloat16)
    blocked = queries.reshape(slots_here, block_rows, row_width)
    arrived = lax.all_to_all(
        jnp.einsum("bn,bkw->nkw", send_table, blocked, preferred_element_type=jnp.float32).astype(
            jnp.bfloat16
        ),
        "seq",
        split_axis=0,
        concat_axis=0,
        tiled=True,
    )
    chosen = jnp.einsum("bn,nkw->bkw", take_table, arrived, preferred_element_type=jnp.float32)
    attended = attend(
        chosen.astype(jnp.bfloat16).reshape(tok_rows, row_width),
        planned_pos,
        key_rows,
        value_rows,
        doc_lengths,
        pair_ids,
    )
    return lax.psum_scatter(
        jnp.dot(attended, out_weight, preferred_element_type=jnp.float32).astype(jnp.bfloat16),
        "head",
        scatter_dimension=0,
        tiled=True,
    )


FAR = 1e9


def cut_columns(width):
    return max(c for c in (1, 2, 4) if width % (c * 128) == 0)


def fused_kernel(
    seq_count,
    head_count,
    queries_ref,
    keys_ref,
    values_ref,
    weight_hbm,
    ends_ref,
    lens_ref,
    pairs_ref,
    plan_ref,
    out_ref,
    weight,
    kv_all,
    q_send,
    q_recv,
    q_heads,
    bias,
    attended,
    right_in,
    left_in,
    right_out,
    left_out,
    weight_sem,
    kv_sems,
    q_sems,
    right_sems,
    left_sems,
):
    me = lax.axis_index("seq")
    rank = lax.axis_index("head")
    slots, block_rows, width = queries_ref.shape
    tokens = slots * block_rows
    seq_len = seq_count * tokens
    heads = width // D_HEAD
    shared = head_count // (keys_ref.shape[1] // D_HEAD)
    chunk_rows = tokens // head_count
    tiles = right_in.shape[1]
    tile = right_in.shape[3]

    weight_copy = pltpu.make_async_copy(weight_hbm, weight, weight_sem)
    weight_copy.start()

    barrier = pltpu.get_barrier_semaphore()
    for step in range(1, seq_count):
        pl.semaphore_signal(
            barrier, inc=1, device_id={"seq": lax.rem(me + step, seq_count)}
        )

    @pl.when(rank > 0)
    def _():
        pl.semaphore_signal(barrier, inc=1, device_id={"head": rank - 1})

    @pl.when(rank < head_count - 1)
    def _():
        pl.semaphore_signal(barrier, inc=1, device_id={"head": rank + 1})

    kv_col = pl.ds(pl.multiple_of((rank // shared) * D_HEAD, D_HEAD), D_HEAD)
    kv_all[me, 0] = keys_ref[:, kv_col]
    kv_all[me, 1] = values_ref[:, kv_col]
    for other in range(seq_count):
        local = jnp.int32(0)
        for slot in range(slots):
            offset = plan_ref[other * slots + slot] - me * slots
            local = local + jnp.where((offset >= 0) & (offset < slots), offset, 0)
        q_send[other] = queries_ref[local]
    q_recv[me] = q_send[me]

    edge = jnp.where(rank > 0, 1, 0) + jnp.where(rank < head_count - 1, 1, 0)
    pl.semaphore_wait(barrier, seq_count - 1 + edge)

    def kv_copy(peer, slot, sender):
        return pltpu.make_async_remote_copy(
            src_ref=kv_all.at[slot],
            dst_ref=kv_all.at[slot],
            send_sem=kv_sems.at[0, sender],
            recv_sem=kv_sems.at[1, slot],
            device_id={"seq": peer},
        )

    def q_copy(peer, slot):
        return pltpu.make_async_remote_copy(
            src_ref=q_send.at[peer],
            dst_ref=q_recv.at[slot],
            send_sem=q_sems.at[0, peer],
            recv_sem=q_sems.at[1, slot],
            device_id={"seq": peer},
        )

    partner = me + 1 - 2 * lax.rem(me, 2)
    for step in range(2, seq_count, 2):
        peer = lax.rem(me + step, seq_count)
        kv_copy(peer, me, peer).start()
    kv_copy(partner, me, me).start()
    for step in range(1, seq_count):
        peer = lax.rem(me + step, seq_count)
        q_copy(peer, me).start()

    row = lax.broadcasted_iota(jnp.int32, (tokens, 1), 0)
    position = row
    for slot in range(slots):
        shift = (plan_ref[me * slots + slot] - slot) * block_rows
        here = (row >= slot * block_rows) & (row < (slot + 1) * block_rows)
        position = position + jnp.where(here, shift, 0)
    position = position.astype(jnp.float32)
    ends = ends_ref[...].astype(jnp.float32)
    starts = ends - lens_ref[...].astype(jnp.float32)
    pairs = pairs_ref[...].astype(jnp.float32)
    begun = starts <= position
    own_start = jnp.max(jnp.where(begun, starts, 0.0), axis=1, keepdims=True)
    own_pair = jnp.max(jnp.where(begun, pairs, 0.0), axis=1, keepdims=True)
    same = pairs == own_pair
    first_start = jnp.min(jnp.where(same, starts, FAR), axis=1, keepdims=True)
    first_end = jnp.min(jnp.where(same, ends, FAR), axis=1, keepdims=True)
    for part in range(seq_count):
        key_pos = (
            lax.broadcasted_iota(jnp.int32, (tokens, tokens), 1) + part * tokens
        ).astype(jnp.float32)
        seen = (key_pos <= position) & (
            (key_pos >= own_start) | ((key_pos >= first_start) & (key_pos < first_end))
        )
        bias[part] = jnp.where(seen, 0.0, NEGATIVE)

    for step in range(2, seq_count, 2):
        source = lax.rem(me + seq_count - step, seq_count)
        kv_copy(partner, source, source).wait_recv()
        kv_copy(partner, source, seq_count + source).start()
    for step in range(1, seq_count):
        source = lax.rem(me + seq_count - step, seq_count)
        q_copy(source, source).wait_recv()
    for slot in range(slots):
        block = q_recv[plan_ref[me * slots + slot] // slots]
        for head in range(heads):
            q_heads[head, slot * block_rows : (slot + 1) * block_rows, :] = block[
                :, head * D_HEAD : (head + 1) * D_HEAD
            ]
    kv_copy(partner, partner, me).wait_recv()
    for step in range(2, seq_count, 2):
        source = lax.rem(partner + seq_count - step, seq_count)
        kv_copy(partner, source, source).wait_recv()

    scale = 1.0 / math.sqrt(D_HEAD)

    def one_head(head, carry):
        rows_q = q_heads[head]
        scores = []
        for part in range(seq_count):
            scores.append(
                lax.dot_general(
                    rows_q,
                    kv_all[part, 0],
                    (((1,), (1,)), ((), ())),
                    preferred_element_type=jnp.float32,
                )
                * scale
                + bias[part]
            )
        top = functools.reduce(jnp.maximum, scores)
        top = jnp.max(top, axis=1, keepdims=True)
        total = jnp.zeros((tokens, tokens), jnp.float32)
        summed = jnp.zeros((tokens, D_HEAD), jnp.float32)
        for part in range(seq_count):
            weights = jnp.exp(scores[part] - top)
            total = total + weights
            summed = summed + jnp.dot(
                weights.astype(jnp.bfloat16),
                kv_all[part, 1],
                preferred_element_type=jnp.float32,
            )
        total = jnp.sum(total, axis=1, keepdims=True)
        result = (summed / total).astype(jnp.bfloat16)
        for chunk in range(head_count):
            attended[head, chunk] = result[chunk * chunk_rows : (chunk + 1) * chunk_rows]
        return carry

    lax.fori_loop(0, heads, one_head, 0)
    weight_copy.wait()

    def own_term(chunk, at):
        columns = pl.ds(pl.multiple_of(at * tile, tile), tile)
        rows_a = jnp.concatenate([attended[head, chunk] for head in range(heads)], axis=1)
        return jnp.dot(rows_a, weight[:, columns], preferred_element_type=jnp.float32)

    def right_copy(chunk, at):
        return pltpu.make_async_remote_copy(
            src_ref=right_out.at[chunk, at],
            dst_ref=right_in.at[chunk, at],
            send_sem=right_sems.at[0, chunk, at],
            recv_sem=right_sems.at[1, chunk, at],
            device_id={"head": jnp.minimum(rank + 1, head_count - 1)},
        )

    def left_copy(chunk, at):
        return pltpu.make_async_remote_copy(
            src_ref=left_out.at[chunk, at],
            dst_ref=left_in.at[chunk, at],
            send_sem=left_sems.at[0, chunk, at],
            recv_sem=left_sems.at[1, chunk, at],
            device_id={"head": jnp.maximum(rank - 1, 0)},
        )

    def advance(item, carry):
        step = item // tiles
        at = item - step * tiles
        far = head_count - 1 - step

        @pl.when((far > rank) & (rank == 0))
        def _():
            right_out[far, at] = own_term(far, at).astype(jnp.bfloat16)
            right_copy(far, at).start()

        @pl.when((step < rank) & (rank == head_count - 1))
        def _():
            left_out[step, at] = own_term(step, at).astype(jnp.bfloat16)
            left_copy(step, at).start()

        @pl.when((far > rank) & (rank > 0))
        def _():
            term = own_term(far, at)
            right_copy(far, at).wait_recv()
            right_out[far, at] = (term + right_in[far, at].astype(jnp.float32)).astype(
                jnp.bfloat16
            )
            right_copy(far, at).start()

        @pl.when((step < rank) & (rank < head_count - 1))
        def _():
            term = own_term(step, at)
            left_copy(step, at).wait_recv()
            left_out[step, at] = (term + left_in[step, at].astype(jnp.float32)).astype(
                jnp.bfloat16
            )
            left_copy(step, at).start()

        return carry

    lax.fori_loop(0, (head_count - 1) * tiles, advance, 0)

    def finish(at, carry):
        columns = pl.ds(pl.multiple_of(at * tile, tile), tile)
        term = own_term(rank, at)

        @pl.when(rank == 0)
        def _():
            left_copy(rank, at).wait_recv()
            out_ref[:, columns] = (term + left_in[rank, at].astype(jnp.float32)).astype(
                jnp.bfloat16
            )

        @pl.when(rank == head_count - 1)
        def _():
            right_copy(rank, at).wait_recv()
            out_ref[:, columns] = (term + right_in[rank, at].astype(jnp.float32)).astype(
                jnp.bfloat16
            )

        @pl.when((rank > 0) & (rank < head_count - 1))
        def _():
            right_copy(rank, at).wait_recv()
            left_copy(rank, at).wait_recv()
            out_ref[:, columns] = (
                term
                + right_in[rank, at].astype(jnp.float32)
                + left_in[rank, at].astype(jnp.float32)
            ).astype(jnp.bfloat16)

        return carry

    lax.fori_loop(0, tiles, finish, 0)

    def drain(item, carry):
        step = item // tiles
        at = item - step * tiles

        @pl.when(step > rank)
        def _():
            right_copy(step, at).wait_send()

        @pl.when(step < rank)
        def _():
            left_copy(step, at).wait_send()

        return carry

    lax.fori_loop(0, head_count * tiles, drain, 0)
    for step in range(1, seq_count):
        peer = lax.rem(me + step, seq_count)
        q_copy(peer, me).wait_send()
    for step in range(2, seq_count, 2):
        peer = lax.rem(me + step, seq_count)
        kv_copy(peer, me, peer).wait_send()
        kv_copy(partner, peer, seq_count + peer).wait_send()
    kv_copy(partner, me, me).wait_send()


def fused_device(queries, keys, values, out_weight, doc_lengths, pair_ids, block_plan):
    seq_count = lax.axis_size("seq")
    head_count = lax.axis_size("head")
    tokens, width = queries.shape
    slots = block_plan.shape[0] // seq_count
    block_rows = tokens // slots
    out_width = out_weight.shape[1]
    tiles = cut_columns(out_width)
    tile = out_width // tiles
    chunk_rows = tokens // head_count
    half = jnp.bfloat16
    flow = pltpu.VMEM((head_count, tiles, chunk_rows, tile), half)
    in_vmem = pl.BlockSpec(memory_space=pltpu.VMEM)
    return pl.pallas_call(
        functools.partial(fused_kernel, seq_count, head_count),
        out_shape=jax.ShapeDtypeStruct((chunk_rows, out_width), half),
        in_specs=[
            in_vmem,
            in_vmem,
            in_vmem,
            pl.BlockSpec(memory_space=pl.ANY),
            in_vmem,
            in_vmem,
            in_vmem,
            pl.BlockSpec(memory_space=pltpu.SMEM),
        ],
        out_specs=in_vmem,
        scratch_shapes=[
            pltpu.VMEM(out_weight.shape, half),
            pltpu.VMEM((seq_count, 2, tokens, D_HEAD), half),
            pltpu.VMEM((seq_count, block_rows, width), half),
            pltpu.VMEM((seq_count, block_rows, width), half),
            pltpu.VMEM((width // D_HEAD, tokens, D_HEAD), half),
            pltpu.VMEM((seq_count, tokens, tokens), jnp.float32),
            pltpu.VMEM((width // D_HEAD, head_count, chunk_rows, D_HEAD), half),
            flow,
            flow,
            flow,
            flow,
            pltpu.SemaphoreType.DMA,
            pltpu.SemaphoreType.DMA((2, 2 * seq_count)),
            pltpu.SemaphoreType.DMA((2, seq_count)),
            pltpu.SemaphoreType.DMA((2, head_count, tiles)),
            pltpu.SemaphoreType.DMA((2, head_count, tiles)),
        ],
        compiler_params=pltpu.CompilerParams(
            collective_id=0, has_side_effects=True, vmem_limit_bytes=60000 * 1024
        ),
    )(
        queries.reshape(slots, block_rows, width),
        keys,
        values,
        out_weight,
        jnp.cumsum(doc_lengths)[None],
        doc_lengths[None],
        pair_ids[None],
        block_plan,
    )


def pick_device(queries, keys, values, out_weight, doc_lengths, pair_ids, block_plan):
    seq_count = lax.axis_size("seq")
    tokens = queries.shape[0]
    block_rows = tokens * seq_count // block_plan.shape[0]
    fits = seq_count * tokens * tokens * 4 <= 4 * 1024 * 1024
    aligned = seq_count % 2 == 0 and block_rows % 16 == 0 and (tokens // lax.axis_size("head")) % 16 == 0
    run = fused_device if fits and aligned else on_device
    return run(queries, keys, values, out_weight, doc_lengths, pair_ids, block_plan)


def solution(mesh):
    return jax.shard_map(
        pick_device,
        mesh=mesh,
        in_specs=(P("seq", "head"), P("seq", None), P("seq", None), P("head", None), P(), P(), P()),
        out_specs=P(("seq", "head"), None),
        check_vma=False,
    )
```

```python
import functools
import math

import jax
import jax.numpy as jnp
from jax import lax
from jax.experimental import pallas as pl
from jax.experimental.pallas import tpu as pltpu
from jax.sharding import PartitionSpec as P

D_HEAD = 128


NEGATIVE = -1e30


def token_docs(positions, doc_lengths):
    doc_ends = jnp.cumsum(doc_lengths)
    return jnp.sum((doc_ends[None, :] <= positions[:, None]).astype(jnp.int32), axis=1)


def pair_firsts(docs, pair_ids):
    doc_range = jnp.arange(pair_ids.shape[0], dtype=jnp.int32)
    own_pair = jnp.sum(jnp.where(docs[:, None] == doc_range[None, :], pair_ids[None, :], 0), axis=1)
    return jnp.sum((pair_ids[None, :] < own_pair[:, None]).astype(jnp.int32), axis=1)


def largest_divisor(total_rows, ceiling):
    return max(
        (
            candidate
            for candidate in range(1, min(total_rows, ceiling) + 1)
            if total_rows % candidate == 0
        )
    )


def attend(query_rows, positions, keys, values, doc_lengths, pair_ids):
    head_size = keys.shape[1]
    token_count = query_rows.shape[0]
    query_heads = query_rows.shape[1] // head_size
    shaped_queries = query_rows.reshape(token_count, query_heads, head_size)
    query_docs = token_docs(positions, doc_lengths)
    query_firsts = pair_firsts(query_docs, pair_ids)
    doc_range = jnp.arange(doc_lengths.shape[0], dtype=jnp.int32)
    pair_begin = jnp.sum(
        jnp.where(doc_range[None, :] < query_firsts[:, None], doc_lengths[None, :], 0), axis=1
    )
    lowest = jnp.min(pair_begin)
    highest = jnp.max(positions)
    scale = 1.0 / math.sqrt(head_size)

    def update(softmax_state, key_block, value_block, block_start):
        key_pos = block_start + jnp.arange(key_block.shape[0], dtype=jnp.int32)
        needed = (block_start <= highest) & (block_start + key_block.shape[0] > lowest)

        def compute(current):
            running_max, denominator, weighted = current
            key_docs = token_docs(key_pos, doc_lengths)
            allowed = (key_pos[None, :] <= positions[:, None]) & (
                (key_docs[None, :] == query_docs[:, None])
                | (key_docs[None, :] == query_firsts[:, None])
            )
            scores = (
                jnp.einsum(
                    "qhd,kd->hqk", shaped_queries, key_block, preferred_element_type=jnp.float32
                )
                * scale
            )
            newest = jnp.maximum(
                running_max, jnp.max(jnp.where(allowed[None], scores, NEGATIVE), axis=2)
            )
            weights = jnp.where(allowed[None], jnp.exp(scores - newest[:, :, None]), 0.0)
            factor = jnp.exp(running_max - newest)
            denominator = denominator * factor + jnp.sum(weights, axis=2)
            weighted = weighted * factor[:, :, None] + jnp.einsum(
                "hqk,kd->hqd",
                weights.astype(jnp.bfloat16),
                value_block,
                preferred_element_type=jnp.float32,
            )
            return (newest, denominator, weighted)

        def unchanged(current):
            return current

        return lax.cond(needed, compute, unchanged, softmax_state)

    initial = (
        jnp.full((query_heads, token_count), NEGATIVE, jnp.float32),
        jnp.zeros((query_heads, token_count), jnp.float32),
        jnp.zeros((query_heads, token_count, head_size), jnp.float32),
    )
    key_rows = lax.all_gather(keys, "seq", axis=0, tiled=True)
    value_rows = lax.all_gather(values, "seq", axis=0, tiled=True)
    row_total = key_rows.shape[0]
    block_rows = largest_divisor(row_total, 1024)
    block_count = row_total // block_rows
    stacked = (
        key_rows.reshape(block_count, block_rows, head_size),
        value_rows.reshape(block_count, block_rows, head_size),
        jnp.int32(0) + block_rows * jnp.arange(block_count, dtype=jnp.int32),
    )

    def advance(carried, block_item):
        return (update(carried, block_item[0], block_item[1], block_item[2]), None)

    result_state, unused_out = lax.scan(advance, initial, stacked)
    running_max, denominator, weighted = result_state
    attended = weighted / denominator[:, :, None]
    return (
        attended.transpose(1, 0, 2)
        .reshape(token_count, query_heads * head_size)
        .astype(jnp.bfloat16)
    )


def on_device(queries, keys, values, out_weight, doc_lengths, pair_ids, block_plan):
    seq_count = lax.axis_size("seq")
    my_seq = lax.axis_index("seq")
    shared_head = lax.axis_index("head") // 2
    key_rows = lax.dynamic_slice_in_dim(keys, shared_head * D_HEAD, D_HEAD, 1)
    value_rows = lax.dynamic_slice_in_dim(values, shared_head * D_HEAD, D_HEAD, 1)
    slots_here = seq_count // 2
    tok_rows = queries.shape[0]
    row_width = queries.shape[1]
    block_rows = tok_rows // slots_here
    slot_total = block_plan.shape[0]
    local_ids = my_seq * slots_here + jnp.arange(slots_here, dtype=jnp.int32)
    plan_rows = lax.dynamic_slice_in_dim(block_plan, my_seq * slots_here, slots_here, 0)
    planned_pos = (
        plan_rows[:, None] * block_rows + jnp.arange(block_rows, dtype=jnp.int32)[None, :]
    ).reshape(-1)
    slot_range = jnp.arange(slot_total, dtype=jnp.int32)
    target_slot = jnp.sum(
        jnp.where(block_plan[None, :] == local_ids[:, None], slot_range[None, :], 0), axis=1
    )
    device_range = jnp.arange(seq_count, dtype=jnp.int32)
    send_table = ((target_slot // slots_here)[:, None] == device_range[None, :]).astype(
        jnp.bfloat16
    )
    take_table = ((plan_rows // slots_here)[:, None] == device_range[None, :]).astype(jnp.bfloat16)
    blocked = queries.reshape(slots_here, block_rows, row_width)
    arrived = lax.all_to_all(
        jnp.einsum("bn,bkw->nkw", send_table, blocked, preferred_element_type=jnp.float32).astype(
            jnp.bfloat16
        ),
        "seq",
        split_axis=0,
        concat_axis=0,
        tiled=True,
    )
    chosen = jnp.einsum("bn,nkw->bkw", take_table, arrived, preferred_element_type=jnp.float32)
    attended = attend(
        chosen.astype(jnp.bfloat16).reshape(tok_rows, row_width),
        planned_pos,
        key_rows,
        value_rows,
        doc_lengths,
        pair_ids,
    )
    return lax.psum_scatter(
        jnp.dot(attended, out_weight, preferred_element_type=jnp.float32).astype(jnp.bfloat16),
        "head",
        scatter_dimension=0,
        tiled=True,
    )


FAR = 1e9


def cut_columns(width):
    return max(c for c in (1, 2, 4) if width % (c * 128) == 0)


def fused_kernel(
    seq_count,
    head_count,
    queries_ref,
    keys_ref,
    values_ref,
    weight_hbm,
    ends_ref,
    lens_ref,
    pairs_ref,
    plan_ref,
    out_ref,
    weight,
    kv_all,
    q_send,
    q_recv,
    q_heads,
    bias,
    attended,
    right_in,
    left_in,
    right_out,
    left_out,
    weight_sem,
    kv_sems,
    q_sems,
    right_sems,
    left_sems,
):
    me = lax.axis_index("seq")
    rank = lax.axis_index("head")
    slots, block_rows, width = queries_ref.shape
    tokens = slots * block_rows
    seq_len = seq_count * tokens
    heads = width // D_HEAD
    shared = head_count // (keys_ref.shape[1] // D_HEAD)
    chunk_rows = tokens // head_count
    tiles = right_in.shape[1]
    tile = right_in.shape[3]

    weight_copy = pltpu.make_async_copy(weight_hbm, weight, weight_sem)
    weight_copy.start()

    barrier = pltpu.get_barrier_semaphore()
    for step in range(1, seq_count):
        pl.semaphore_signal(
            barrier, inc=1, device_id={"seq": lax.rem(me + step, seq_count)}
        )

    @pl.when(rank > 0)
    def _():
        pl.semaphore_signal(barrier, inc=1, device_id={"head": rank - 1})

    @pl.when(rank < head_count - 1)
    def _():
        pl.semaphore_signal(barrier, inc=1, device_id={"head": rank + 1})

    kv_col = pl.ds(pl.multiple_of((rank // shared) * D_HEAD, D_HEAD), D_HEAD)
    kv_all[me, 0] = keys_ref[:, kv_col]
    kv_all[me, 1] = values_ref[:, kv_col]
    for other in range(seq_count):
        local = jnp.int32(0)
        for slot in range(slots):
            offset = plan_ref[other * slots + slot] - me * slots
            local = local + jnp.where((offset >= 0) & (offset < slots), offset, 0)
        q_send[other] = queries_ref[local]
    q_recv[me] = q_send[me]

    edge = jnp.where(rank > 0, 1, 0) + jnp.where(rank < head_count - 1, 1, 0)
    pl.semaphore_wait(barrier, seq_count - 1 + edge)

    def kv_copy(peer, slot, sender):
        return pltpu.make_async_remote_copy(
            src_ref=kv_all.at[slot],
            dst_ref=kv_all.at[slot],
            send_sem=kv_sems.at[0, sender],
            recv_sem=kv_sems.at[1, slot],
            device_id={"seq": peer},
        )

    def q_copy(peer, slot):
        return pltpu.make_async_remote_copy(
            src_ref=q_send.at[peer],
            dst_ref=q_recv.at[slot],
            send_sem=q_sems.at[0, peer],
            recv_sem=q_sems.at[1, slot],
            device_id={"seq": peer},
        )

    partner = me + 1 - 2 * lax.rem(me, 2)
    for step in range(2, seq_count, 2):
        peer = lax.rem(me + step, seq_count)
        kv_copy(peer, me, peer).start()
    kv_copy(partner, me, me).start()
    for step in range(1, seq_count):
        peer = lax.rem(me + step, seq_count)
        q_copy(peer, me).start()

    row = lax.broadcasted_iota(jnp.int32, (tokens, 1), 0)
    position = row
    for slot in range(slots):
        shift = (plan_ref[me * slots + slot] - slot) * block_rows
        here = (row >= slot * block_rows) & (row < (slot + 1) * block_rows)
        position = position + jnp.where(here, shift, 0)
    position = position.astype(jnp.float32)
    ends = ends_ref[...].astype(jnp.float32)
    starts = ends - lens_ref[...].astype(jnp.float32)
    pairs = pairs_ref[...].astype(jnp.float32)
    begun = starts <= position
    own_start = jnp.max(jnp.where(begun, starts, 0.0), axis=1, keepdims=True)
    own_pair = jnp.max(jnp.where(begun, pairs, 0.0), axis=1, keepdims=True)
    same = pairs == own_pair
    first_start = jnp.min(jnp.where(same, starts, FAR), axis=1, keepdims=True)
    first_end = jnp.min(jnp.where(same, ends, FAR), axis=1, keepdims=True)
    for part in range(seq_count):
        key_pos = (
            lax.broadcasted_iota(jnp.int32, (tokens, tokens), 1) + part * tokens
        ).astype(jnp.float32)
        seen = (key_pos <= position) & (
            (key_pos >= own_start) | ((key_pos >= first_start) & (key_pos < first_end))
        )
        bias[part] = jnp.where(seen, 0.0, NEGATIVE)

    for step in range(2, seq_count, 2):
        source = lax.rem(me + seq_count - step, seq_count)
        kv_copy(partner, source, source).wait_recv()
        kv_copy(partner, source, seq_count + source).start()
    for step in range(1, seq_count):
        source = lax.rem(me + seq_count - step, seq_count)
        q_copy(source, source).wait_recv()
    for slot in range(slots):
        block = q_recv[plan_ref[me * slots + slot] // slots]
        for head in range(heads):
            q_heads[slot, head * block_rows : (head + 1) * block_rows, :] = block[
                :, head * D_HEAD : (head + 1) * D_HEAD
            ]
    kv_copy(partner, partner, me).wait_recv()
    for step in range(2, seq_count, 2):
        source = lax.rem(partner + seq_count - step, seq_count)
        kv_copy(partner, source, source).wait_recv()

    scale = 1.0 / math.sqrt(D_HEAD)

    weight_copy.wait()

    def own_term(chunk, at):
        columns = pl.ds(at * tile if isinstance(at, int) else pl.multiple_of(at * tile, tile), tile)
        rows_a = jnp.concatenate([attended[head, chunk] for head in range(heads)], axis=1)
        return jnp.dot(rows_a, weight[:, columns], preferred_element_type=jnp.float32)

    def right_copy(chunk, at):
        return pltpu.make_async_remote_copy(
            src_ref=right_out.at[chunk, at],
            dst_ref=right_in.at[chunk, at],
            send_sem=right_sems.at[0, chunk, at],
            recv_sem=right_sems.at[1, chunk, at],
            device_id={"head": jnp.minimum(rank + 1, head_count - 1)},
        )

    def left_copy(chunk, at):
        return pltpu.make_async_remote_copy(
            src_ref=left_out.at[chunk, at],
            dst_ref=left_in.at[chunk, at],
            send_sem=left_sems.at[0, chunk, at],
            recv_sem=left_sems.at[1, chunk, at],
            device_id={"head": jnp.maximum(rank - 1, 0)},
        )

    def one_chunk(turn, carry):
        chunk = jnp.where(rank < head_count // 2, head_count - 1 - turn, turn)
        rows_q = q_heads[chunk]
        rows_at = pl.ds(pl.multiple_of(chunk * chunk_rows, chunk_rows), chunk_rows)
        scores = []
        for part in range(seq_count):
            scores.append(
                lax.dot_general(
                    rows_q,
                    kv_all[part, 0],
                    (((1,), (1,)), ((), ())),
                    preferred_element_type=jnp.float32,
                )
                * scale
                + jnp.concatenate([bias[part, rows_at, :]] * heads, axis=0)
            )
        top = functools.reduce(jnp.maximum, scores)
        top = jnp.max(top, axis=1, keepdims=True)
        total = jnp.zeros((heads * chunk_rows, tokens), jnp.float32)
        summed = jnp.zeros((heads * chunk_rows, D_HEAD), jnp.float32)
        for part in range(seq_count):
            weights = jnp.exp(scores[part] - top)
            total = total + weights
            summed = summed + jnp.dot(
                weights.astype(jnp.bfloat16),
                kv_all[part, 1],
                preferred_element_type=jnp.float32,
            )
        total = jnp.sum(total, axis=1, keepdims=True)
        result = (summed / total).astype(jnp.bfloat16)
        for head in range(heads):
            attended[head, chunk] = result[head * chunk_rows : (head + 1) * chunk_rows]

        @pl.when((rank == 0) & (chunk > 0))
        def _():
            for at in range(tiles):
                right_out[chunk, at] = own_term(chunk, at).astype(jnp.bfloat16)
                right_copy(chunk, at).start()

        @pl.when((rank == head_count - 1) & (chunk < rank))
        def _():
            for at in range(tiles):
                left_out[chunk, at] = own_term(chunk, at).astype(jnp.bfloat16)
                left_copy(chunk, at).start()

        return carry

    lax.fori_loop(0, head_count, one_chunk, 0)

    def advance(item, carry):
        step = item // tiles
        at = item - step * tiles
        far = head_count - 1 - step

        @pl.when((far > rank) & (rank > 0))
        def _():
            term = own_term(far, at)
            right_copy(far, at).wait_recv()
            right_out[far, at] = (term + right_in[far, at].astype(jnp.float32)).astype(
                jnp.bfloat16
            )
            right_copy(far, at).start()

        @pl.when((step < rank) & (rank < head_count - 1))
        def _():
            term = own_term(step, at)
            left_copy(step, at).wait_recv()
            left_out[step, at] = (term + left_in[step, at].astype(jnp.float32)).astype(
                jnp.bfloat16
            )
            left_copy(step, at).start()

        return carry

    lax.fori_loop(0, (head_count - 1) * tiles, advance, 0)

    def finish(at, carry):
        columns = pl.ds(pl.multiple_of(at * tile, tile), tile)
        term = own_term(rank, at)

        @pl.when(rank == 0)
        def _():
            left_copy(rank, at).wait_recv()
            out_ref[:, columns] = (term + left_in[rank, at].astype(jnp.float32)).astype(
                jnp.bfloat16
            )

        @pl.when(rank == head_count - 1)
        def _():
            right_copy(rank, at).wait_recv()
            out_ref[:, columns] = (term + right_in[rank, at].astype(jnp.float32)).astype(
                jnp.bfloat16
            )

        @pl.when((rank > 0) & (rank < head_count - 1))
        def _():
            right_copy(rank, at).wait_recv()
            left_copy(rank, at).wait_recv()
            out_ref[:, columns] = (
                term
                + right_in[rank, at].astype(jnp.float32)
                + left_in[rank, at].astype(jnp.float32)
            ).astype(jnp.bfloat16)

        return carry

    lax.fori_loop(0, tiles, finish, 0)

    def drain(item, carry):
        step = item // tiles
        at = item - step * tiles

        @pl.when(step > rank)
        def _():
            right_copy(step, at).wait_send()

        @pl.when(step < rank)
        def _():
            left_copy(step, at).wait_send()

        return carry

    lax.fori_loop(0, head_count * tiles, drain, 0)
    for step in range(1, seq_count):
        peer = lax.rem(me + step, seq_count)
        q_copy(peer, me).wait_send()
    for step in range(2, seq_count, 2):
        peer = lax.rem(me + step, seq_count)
        kv_copy(peer, me, peer).wait_send()
        kv_copy(partner, peer, seq_count + peer).wait_send()
    kv_copy(partner, me, me).wait_send()


def fused_device(queries, keys, values, out_weight, doc_lengths, pair_ids, block_plan):
    seq_count = lax.axis_size("seq")
    head_count = lax.axis_size("head")
    tokens, width = queries.shape
    slots = block_plan.shape[0] // seq_count
    block_rows = tokens // slots
    out_width = out_weight.shape[1]
    tiles = cut_columns(out_width)
    tile = out_width // tiles
    chunk_rows = tokens // head_count
    half = jnp.bfloat16
    flow = pltpu.VMEM((head_count, tiles, chunk_rows, tile), half)
    in_vmem = pl.BlockSpec(memory_space=pltpu.VMEM)
    return pl.pallas_call(
        functools.partial(fused_kernel, seq_count, head_count),
        out_shape=jax.ShapeDtypeStruct((chunk_rows, out_width), half),
        in_specs=[
            in_vmem,
            in_vmem,
            in_vmem,
            pl.BlockSpec(memory_space=pl.ANY),
            in_vmem,
            in_vmem,
            in_vmem,
            pl.BlockSpec(memory_space=pltpu.SMEM),
        ],
        out_specs=in_vmem,
        scratch_shapes=[
            pltpu.VMEM(out_weight.shape, half),
            pltpu.VMEM((seq_count, 2, tokens, D_HEAD), half),
            pltpu.VMEM((seq_count, block_rows, width), half),
            pltpu.VMEM((seq_count, block_rows, width), half),
            pltpu.VMEM((slots, width // D_HEAD * block_rows, D_HEAD), half),
            pltpu.VMEM((seq_count, tokens, tokens), jnp.float32),
            pltpu.VMEM((width // D_HEAD, head_count, chunk_rows, D_HEAD), half),
            flow,
            flow,
            flow,
            flow,
            pltpu.SemaphoreType.DMA,
            pltpu.SemaphoreType.DMA((2, 2 * seq_count)),
            pltpu.SemaphoreType.DMA((2, seq_count)),
            pltpu.SemaphoreType.DMA((2, head_count, tiles)),
            pltpu.SemaphoreType.DMA((2, head_count, tiles)),
        ],
        compiler_params=pltpu.CompilerParams(
            collective_id=0, has_side_effects=True, vmem_limit_bytes=60000 * 1024
        ),
    )(
        queries.reshape(slots, block_rows, width),
        keys,
        values,
        out_weight,
        jnp.cumsum(doc_lengths)[None],
        doc_lengths[None],
        pair_ids[None],
        block_plan,
    )


def pick_device(queries, keys, values, out_weight, doc_lengths, pair_ids, block_plan):
    seq_count = lax.axis_size("seq")
    tokens = queries.shape[0]
    block_rows = tokens * seq_count // block_plan.shape[0]
    fits = seq_count * tokens * tokens * 4 <= 4 * 1024 * 1024
    square = block_rows * lax.axis_size("head") == tokens
    aligned = square and seq_count % 2 == 0 and block_rows % 16 == 0 and (tokens // lax.axis_size("head")) % 16 == 0
    run = fused_device if fits and aligned else on_device
    return run(queries, keys, values, out_weight, doc_lengths, pair_ids, block_plan)


def solution(mesh):
    return jax.shard_map(
        pick_device,
        mesh=mesh,
        in_specs=(P("seq", "head"), P("seq", None), P("seq", None), P("head", None), P(), P(), P()),
        out_specs=P(("seq", "head"), None),
        check_vma=False,
    )
```
